32 devices in a mesh: seq: 16 (over z, x, core), chan: 2 (over y).
Axes of the slice: x: 2, y: 2, z: 4, core: 2. Of those that a mesh axis runs over, the one named last changes fastest.
Arguments:
- signal: bfloat16 [524288, 256], P('seq', 'chan'), parts along dimension 1, may hold values from -6 to 6
- gate_values: bfloat16 [524288, 256], P('seq', 'chan'), parts along dimension 1, may hold values from -4 to 4
- skip_gain: float32 [256], P('chan'), parts along dimension 0, may hold values from 0.25 to 2
- filter_spectrum: bfloat16 [2, 512, 1024, 256], P(None, 'seq', None, 'chan'), parts along dimension 3, may hold values from -4 to 4, as said below
Outputs:
- gated_output: bfloat16 [524288, 256], P('seq', 'chan'), parts along dimension 1
The draws below stay inside these ranges and needn't reach their ends.
There are 2 independent parts, one for each index of `chan`. The reference program is written for one: setup_inputs(seed, part) draws one part's arguments, and reference() takes and returns one part's arrays. A program takes and returns all parts, laid end to end along the dimension named above; each array names one. Nothing has to cross between parts.
Inputs may be any that keep to these rules, and one draw needn't show every extreme that they name: `filter_spectrum`: the spectrum of a real filter: the complex entry at frequency k equals the conjugate of the entry at frequency (524288 - k) mod 524288.
All inputs are finite; a program needn't handle non-finite values.
Results may differ from the reference program's by a relative error of at most 0.0085.
Values may be sent and summed in bfloat16 or wider, within the bound.
A program may use at most 256 MiB of HBM per device.

```python
import math
import jax
import jax.numpy as jnp
from jax import lax

OUTER = 1024
INNER = 512
CH = 128
SEQ = 524288


def draw_filter_spectrum(key, part):
    length = INNER * OUTER
    first_key = jax.random.fold_in(key, 11)
    base = jax.random.normal(first_key, (2, length, CH), jnp.float32)
    mirror = jnp.roll(jnp.flip(base, axis=1), 1, axis=1)
    real_part = (base[0] + mirror[0]) * 0.7071
    imag_part = (base[1] - mirror[1]) * 0.7071
    both = jnp.clip(jnp.stack([real_part, imag_part]), -4.0, 4.0)
    return both.reshape(2, INNER, OUTER, CH).astype(jnp.bfloat16)


def level_of(rng, extent, split, smallest, top_value):
    factor_of = 1.0
    for axis_at, blocks in split:
        heights = jax.random.uniform(jax.random.fold_in(jax.random.fold_in(rng, 6), axis_at), (blocks,), jnp.float32, smallest / len(split), top_value / len(split))
        factor_of = factor_of * jnp.repeat(jnp.exp(heights), extent[axis_at] // blocks).reshape((-1,) + (1,) * (len(extent) - 1 - axis_at))
    return factor_of


def centred(rng, extent, scale, limit, cuts=(), held_as=jnp.bfloat16):
    level = level_of(rng, extent, cuts, -0.22, 0.18) if cuts else 1.0
    values = jax.random.normal(rng, extent, jnp.float32) * scale * level
    return jnp.minimum(jnp.maximum(values, -limit), limit).astype(held_as)


def setup_inputs(seed: int = 0, part: int = 0) -> dict:
    keys = jax.random.split(jax.random.key(seed), 5)
    part_keys = jax.random.split(jax.random.fold_in(keys[4], part), 5)
    signal = centred(part_keys[0], (SEQ, CH), 1.0, 6.0, ((0, 16),))
    gate_values = centred(part_keys[1], (SEQ, CH), 1.0, 4.0, ((0, 16),))
    skip_gain = jnp.clip(jnp.exp(jax.random.uniform(part_keys[2], (CH,), jnp.float32, math.log(0.25), math.log(2.0))), 0.25, 2.0)
    filter_spectrum = draw_filter_spectrum(jax.random.fold_in(jax.random.fold_in(keys[4], part), 71), part)
    return {"signal": signal, "gate_values": gate_values, "skip_gain": skip_gain, "filter_spectrum": filter_spectrum}


def tables(length):
    indices = lax.iota(jnp.int32, length)
    angles = 2.0 * math.pi / length * (indices[:, None] * indices[None, :] % length).astype(jnp.float32)
    return (jnp.cos(angles).astype(jnp.bfloat16), jnp.sin(angles).astype(jnp.bfloat16))

def twiddle(c_values, b_values, length):
    angles = 2.0 * math.pi / length * (c_values[:, None] * b_values[None, :] % length).astype(jnp.float32)
    return (jnp.cos(angles), jnp.sin(angles))

def convolve(operands):
    pieces, filter_cols = operands
    cos_a, sin_a = tables(OUTER)
    cos_b, sin_b = tables(INNER)
    inner_table = jnp.stack([cos_b, sin_b]).astype(jnp.float32)
    tw_cos, tw_sin = twiddle(lax.iota(jnp.int32, OUTER), lax.iota(jnp.int32, INNER), SEQ)
    tw_cos = tw_cos[:, :, None]
    tw_sin = tw_sin[:, :, None]
    outer_scale = 1.0 / math.sqrt(OUTER)
    inner_scale = 1.0 / math.sqrt(INNER)
    breadth = pieces.shape[2]
    flattened = pieces.reshape(OUTER, INNER * breadth)
    fwd_re = jnp.dot(cos_a, flattened, preferred_element_type=jnp.float32).reshape(OUTER, INNER, breadth)
    fwd_im = -jnp.dot(sin_a, flattened, preferred_element_type=jnp.float32).reshape(OUTER, INNER, breadth)
    twisted = jnp.stack([(fwd_re * tw_cos + fwd_im * tw_sin) * outer_scale, (fwd_im * tw_cos - fwd_re * tw_sin) * outer_scale]).astype(jnp.bfloat16)
    partials = jnp.einsum('tdb,scbk->tscdk', inner_table, twisted.astype(jnp.float32), precision=lax.Precision.HIGHEST)
    spectrum = jnp.stack([(partials[0, 0] + partials[1, 1]) * inner_scale, (partials[0, 1] - partials[1, 0]) * inner_scale]).astype(jnp.bfloat16)
    filter_re = jnp.swapaxes(filter_cols[0], 0, 1).astype(jnp.float32)
    filter_im = jnp.swapaxes(filter_cols[1], 0, 1).astype(jnp.float32)
    spec_re = spectrum[0].astype(jnp.float32)
    spec_im = spectrum[1].astype(jnp.float32)
    product = jnp.stack([spec_re * filter_re - spec_im * filter_im, spec_re * filter_im + spec_im * filter_re]).astype(jnp.bfloat16)
    partials = jnp.einsum('tbd,scdk->tscbk', inner_table, product.astype(jnp.float32), precision=lax.Precision.HIGHEST)
    back_re = (partials[0, 0] - partials[1, 1]) * inner_scale
    back_im = (partials[0, 1] + partials[1, 0]) * inner_scale
    rotated_re = (back_re * tw_cos - back_im * tw_sin).astype(jnp.bfloat16)
    rotated_im = (back_re * tw_sin + back_im * tw_cos).astype(jnp.bfloat16)
    convolved = (jnp.dot(cos_a, rotated_re.reshape(OUTER, INNER * breadth), preferred_element_type=jnp.float32) - jnp.dot(sin_a, rotated_im.reshape(OUTER, INNER * breadth), preferred_element_type=jnp.float32)) * outer_scale
    return convolved.reshape(OUTER, INNER, breadth).astype(jnp.bfloat16)

def reference(signal, gate_values, skip_gain, filter_spectrum):
    channels = signal.shape[1]
    group_width = 16 if channels % 16 == 0 else channels
    groups = channels // group_width
    signal_grid = signal.reshape(OUTER, INNER, groups, group_width).transpose(2, 0, 1, 3)
    filter_grid = filter_spectrum.reshape(2, INNER, OUTER, groups, group_width).transpose(3, 0, 1, 2, 4)
    convolved = lax.map(convolve, (signal_grid, filter_grid))
    convolved = convolved.transpose(1, 2, 0, 3).reshape(SEQ, channels)
    result = gate_values.astype(jnp.float32) * (convolved.astype(jnp.float32) + skip_gain[None, :].astype(jnp.float32) * signal.astype(jnp.float32))
    return result.astype(jnp.bfloat16)
```

```python
import math

import jax
import jax.numpy as jnp
from jax import lax
from jax.experimental import pallas as pl
from jax.experimental.pallas import tpu as pltpu
from jax.sharding import PartitionSpec as P

MESH = pl.DeviceIdType.MESH


def tables(length, rows=None, columns=None):
    rows = lax.iota(jnp.int32, length) if rows is None else rows
    columns = lax.iota(jnp.int32, length) if columns is None else columns
    angles = 2.0 * math.pi / length * (rows[:, None] * columns[None, :] % length).astype(jnp.float32)
    return (jnp.cos(angles).astype(jnp.bfloat16), jnp.sin(angles).astype(jnp.bfloat16))


def twiddle(c_values, b_values, length):
    angles = (
        2.0
        * math.pi
        / length
        * (c_values[:, None] * b_values[None, :] % length).astype(jnp.float32)
    )
    return (jnp.cos(angles), jnp.sin(angles))


def flip(me, i, shards):
    out, bit = 0, 1
    while bit < shards:
        out = out + lax.rem(lax.div(me, bit) + lax.div(i, bit), 2) * bit
        bit *= 2
    return out


def matmul(a, b):
    return lax.dot_general(a, b, (((1,), (0,)), ((), ())), preferred_element_type=jnp.float32)


def matmul_nt(a, b):
    return lax.dot_general(a, b, (((1,), (1,)), ((), ())), preferred_element_type=jnp.float32)


def convolve(sig, filt, ext, outer, fwd, inv, tw_cb, tw_bc, shards):
    ch_loc, a_loc, inner = sig.shape[1:]
    d_loc, n_outer = filt.shape[3:]
    half = shards // 2
    d_half = half * d_loc
    step = 256
    chunks = n_outer // step
    inner_scale = 1.0 / math.sqrt(inner)
    ahead = min(3, ch_loc)
    last = pl.ds(0, shards - 1)

    def kernel(
        sig_ref, filt_ref, ext_ref, outer_ref, fwd_ref, inv_ref, tcb_ref, tbc_ref, conv_ref,
        s_buf, f_buf, e_buf, outer_t, fwd_t, inv_t, tcb, tbc, r_buf, o_buf,
        sig_send, sig_recv, filt_send, filt_recv, ext_send, ext_recv,
        out_send, out_recv, table_sem,
    ):
        me = lax.axis_index("seq")
        side = lax.div(me, half)
        mine = lax.rem(me, half)
        barrier = pltpu.get_barrier_semaphore()

        def greet(i, carry):
            pl.semaphore_signal(
                barrier, inc=1, device_id={"seq": lax.rem(me + i, shards)}, device_id_type=MESH
            )
            return carry

        lax.fori_loop(1, shards, greet, 0)
        pl.semaphore_wait(barrier, shards - 1)

        def rows(s):
            return pl.ds(pl.multiple_of(s * a_loc, a_loc), a_loc)

        def send_round(k):
            def send_signal(i, carry):
                to = flip(me, shards - i, shards)
                pltpu.make_async_remote_copy(
                    src_ref=sig_ref.at[to, k],
                    dst_ref=s_buf.at[k, rows(me)],
                    send_sem=sig_send.at[k],
                    recv_sem=sig_recv.at[k],
                    device_id={"seq": to},
                    device_id_type=MESH,
                ).start()
                return carry

            def send_filter(i, carry):
                to = flip(me, half - i, shards)
                pltpu.make_async_remote_copy(
                    src_ref=filt_ref.at[to, k],
                    dst_ref=f_buf.at[k, :, mine],
                    send_sem=filt_send.at[k],
                    recv_sem=filt_recv.at[k],
                    device_id={"seq": to},
                    device_id_type=MESH,
                ).start()
                return carry

            lax.fori_loop(1, shards, send_signal, 0)
            lax.fori_loop(1, half, send_filter, 0)
            pltpu.make_async_copy(sig_ref.at[me, k], s_buf.at[k, rows(me)], sig_recv.at[k]).start()
            pltpu.make_async_copy(filt_ref.at[me, k], f_buf.at[k, :, mine], filt_recv.at[k]).start()

        @pl.when(mine == 0)
        def _():
            def send_ext(i, carry):
                to = (1 - side) * half + i
                pltpu.make_async_remote_copy(
                    src_ref=ext_ref.at[to],
                    dst_ref=e_buf,
                    send_sem=ext_send,
                    recv_sem=ext_recv,
                    device_id={"seq": to},
                    device_id_type=MESH,
                ).start()
                return carry

            lax.fori_loop(0, half, send_ext, 0)

        for k in range(ahead):
            send_round(k)
        loads = [
            pltpu.make_async_copy(src, dst, table_sem.at[i])
            for i, (src, dst) in enumerate(
                [
                    (outer_ref, outer_t),
                    (fwd_ref, fwd_t),
                    (inv_ref, inv_t),
                    (tcb_ref, tcb),
                    (tbc_ref, tbc),
                ]
            )
        ]
        for load in loads:
            load.start()
        for load in loads:
            load.wait()
        pltpu.make_async_copy(e_buf, e_buf, ext_recv).wait()

        b_row = lax.broadcasted_iota(jnp.int32, (1, inner), 1)
        b_col = lax.broadcasted_iota(jnp.int32, (inner, 1), 0)
        swing = (1 - side).astype(jnp.float32)
        sign_row = 1.0 - 2.0 * swing * (b_row % 2).astype(jnp.float32)
        sign_col = 1.0 - 2.0 * swing * (b_col % 2).astype(jnp.float32)

        def channel(k, carry):
            slot = lax.rem(k, 2)

            @pl.when(k + ahead < ch_loc)
            def _():
                send_round(k + ahead)

            pltpu.make_async_copy(s_buf.at[k], s_buf.at[k], sig_recv.at[k]).wait()
            pltpu.make_async_copy(f_buf.at[k], f_buf.at[k], filt_recv.at[k]).wait()
            special = e_buf[k, :, 0:1]

            def forward(j, carry):
                at = pl.multiple_of(j * step, step)
                here = pl.ds(at, step)
                x = s_buf[k]
                f_re = matmul(outer_t[here, :], x)
                f_im = matmul(outer_t[pl.ds(pl.multiple_of(n_outer + at, step), step), :], x)
                cos, sin = tcb[0, here, :], tcb[1, here, :]
                q_re = (f_re * cos + f_im * sin).astype(jnp.bfloat16)
                q_im = (f_im * cos - f_re * sin).astype(jnp.bfloat16)
                q = jnp.concatenate([q_re, q_im], axis=1)
                spectrum = matmul_nt(fwd_t[...], q) * inner_scale
                spectrum = spectrum.astype(jnp.bfloat16).astype(jnp.float32)
                s_re, s_im = spectrum[:d_half], spectrum[d_half:]
                h_re = f_buf[k, 0, :, :, here].astype(jnp.float32).reshape(d_half, step)
                h_im = f_buf[k, 1, :, :, here].astype(jnp.float32).reshape(d_half, step)
                d_at = lax.broadcasted_iota(jnp.int32, (d_half, step), 0)
                c_at = lax.broadcasted_iota(jnp.int32, (d_half, step), 1) + at
                share = jnp.where((d_at == 0) & (c_at == 0), 0.5, 1.0)
                product = jnp.concatenate(
                    [(s_re * h_re - s_im * h_im) * share, (s_re * h_im + s_im * h_re) * share],
                    axis=0,
                ).astype(jnp.bfloat16)
                edge = jnp.sum(q_re[0:1].astype(jnp.float32) * sign_row, axis=1, keepdims=True)
                edge = (edge * inner_scale).astype(jnp.bfloat16).astype(jnp.float32)
                edge = (edge * special).astype(jnp.bfloat16).astype(jnp.float32) * 0.5
                c_row = lax.broadcasted_iota(jnp.int32, (1, step), 1) + at
                edge = jnp.where(c_row == 0, edge, 0.0)
                u = matmul(inv_t[...], product)
                u_re, u_im = u[:inner] + sign_col * edge, u[inner:]
                cos, sin = tbc[0, :, here], tbc[1, :, here]
                r_buf[0, :, here] = (u_re * cos - u_im * sin).astype(jnp.bfloat16)
                r_buf[1, :, here] = (u_re * sin + u_im * cos).astype(jnp.bfloat16)
                return carry

            lax.fori_loop(0, chunks, forward, 0)

            @pl.when(k >= 2)
            def _():
                pltpu.make_async_copy(o_buf.at[slot], o_buf.at[slot], out_send.at[slot]).wait()

            def backward(j, carry):
                at = pl.multiple_of(j * step, step)
                conv = matmul_nt(outer_t[pl.ds(at, step), :], r_buf[0]) + matmul_nt(
                    outer_t[pl.ds(pl.multiple_of(n_outer + at, step), step), :], r_buf[1]
                )
                conv = conv * (2.0 / math.sqrt(n_outer))
                o_buf[slot, pl.ds(at, step), :] = conv.astype(jnp.bfloat16)
                return carry

            lax.fori_loop(0, chunks, backward, 0)
            pltpu.make_async_copy(
                o_buf.at[slot, rows(me)], conv_ref.at[me, k], out_send.at[slot]
            ).start()

            def send_out(i, carry):
                to = flip(me, shards - i, shards)
                pltpu.make_async_remote_copy(
                    src_ref=o_buf.at[slot, rows(to)],
                    dst_ref=conv_ref.at[me, k],
                    send_sem=out_send.at[slot],
                    recv_sem=out_recv,
                    device_id={"seq": to},
                    device_id_type=MESH,
                ).start()
                return carry

            lax.fori_loop(1, shards, send_out, 0)
            return carry

        lax.fori_loop(0, ch_loc, channel, 0)
        for slot in range(min(2, ch_loc)):
            pltpu.make_async_copy(o_buf.at[slot], o_buf.at[slot], out_send.at[slot]).wait()
        for k in range(ch_loc):
            pltpu.make_async_copy(sig_ref.at[last, k], sig_ref.at[last, k], sig_send.at[k]).wait()
            own = filt_ref.at[pl.ds(0, half - 1), k]
            pltpu.make_async_copy(own, own, filt_send.at[k]).wait()

        @pl.when(mine == 0)
        def _():
            own = ext_ref.at[pl.ds(0, half)]
            pltpu.make_async_copy(own, own, ext_send).wait()

        pltpu.make_async_copy(conv_ref.at[last], conv_ref.at[last], out_recv).wait()

    anywhere = pl.BlockSpec(memory_space=pl.ANY)
    bf16 = jnp.bfloat16
    return pl.pallas_call(
        kernel,
        out_shape=jax.ShapeDtypeStruct(sig.shape, bf16),
        in_specs=[anywhere] * 8,
        out_specs=anywhere,
        scratch_shapes=[
            pltpu.VMEM((ch_loc, shards * a_loc, inner), bf16),
            pltpu.VMEM((ch_loc, 2, half, d_loc, n_outer), bf16),
            pltpu.VMEM(ext.shape[1:], jnp.float32),
            pltpu.VMEM(outer.shape, bf16),
            pltpu.VMEM(fwd.shape, bf16),
            pltpu.VMEM(inv.shape, bf16),
            pltpu.VMEM(tw_cb.shape, jnp.float32),
            pltpu.VMEM(tw_bc.shape, jnp.float32),
            pltpu.VMEM((2, inner, n_outer), bf16),
            pltpu.VMEM((2, n_outer, inner), bf16),
            pltpu.SemaphoreType.DMA((ch_loc,)),
            pltpu.SemaphoreType.DMA((ch_loc,)),
            pltpu.SemaphoreType.DMA((ch_loc,)),
            pltpu.SemaphoreType.DMA((ch_loc,)),
            pltpu.SemaphoreType.DMA,
            pltpu.SemaphoreType.DMA,
            pltpu.SemaphoreType.DMA((2,)),
            pltpu.SemaphoreType.DMA,
            pltpu.SemaphoreType.DMA((5,)),
        ],
        compiler_params=pltpu.CompilerParams(
            collective_id=0, has_side_effects=True, vmem_limit_bytes=63 * 1024 * 1024
        ),
        name="convolve",
    )(sig, filt, ext, outer, fwd, inv, tw_cb, tw_bc)


def local(signal, gate_values, skip_gain, filter_spectrum):
    shards = lax.axis_size("seq")
    me = lax.axis_index("seq")
    positions, channels = signal.shape
    d_loc, n_outer = filter_spectrum.shape[1:3]
    inner = d_loc * shards
    length = n_outer * inner
    ch_loc = channels // shards
    a_loc = n_outer // shards
    half = shards // 2
    side = me // half
    outer_scale = 1.0 / math.sqrt(n_outer)
    inner_scale = 1.0 / math.sqrt(inner)

    cos_a, sin_a = tables(n_outer)
    outer = jnp.concatenate([cos_a, -sin_a], 0)
    d_values = side * (inner // 2) + lax.iota(jnp.int32, inner // 2)
    cos_b, sin_b = tables(inner, d_values)
    fwd = jnp.concatenate(
        [jnp.concatenate([cos_b, sin_b], 1), jnp.concatenate([-sin_b, cos_b], 1)], 0
    )
    inv = fwd.T
    cos, sin = twiddle(lax.iota(jnp.int32, n_outer), lax.iota(jnp.int32, inner), length)
    tw_cb = jnp.stack([cos, sin]) * outer_scale
    tw_bc = jnp.stack([cos.T, sin.T]) * inner_scale

    sig = signal.T.reshape(shards, ch_loc, a_loc, inner)
    filt = filter_spectrum.transpose(3, 0, 1, 2).reshape(shards, ch_loc, 2, d_loc, n_outer)
    ext = jnp.broadcast_to(
        filter_spectrum[0, 0, 0].astype(jnp.float32).reshape(shards, ch_loc, 1, 1),
        (shards, ch_loc, 1, 128),
    )
    convolved = convolve(sig, filt, ext, outer, fwd, inv, tw_cb, tw_bc, shards)
    convolved = convolved.reshape(channels, positions).T
    result = gate_values.astype(jnp.float32) * (
        convolved.astype(jnp.float32) + skip_gain[None, :] * signal.astype(jnp.float32)
    )
    return result.astype(jnp.bfloat16)


def solution(mesh):
    return jax.shard_map(
        local,
        mesh=mesh,
        in_specs=(P("seq", "chan"), P("seq", "chan"), P("chan"), P(None, "seq", None, "chan")),
        out_specs=P("seq", "chan"),
        check_vma=False,
    )
```

```python
import math

import jax
import jax.numpy as jnp
from jax import lax
from jax.experimental import pallas as pl
from jax.experimental.pallas import tpu as pltpu
from jax.sharding import PartitionSpec as P

MESH = pl.DeviceIdType.MESH
LANES = 128
GROUP = 16
PITCH = 24
STRIDE = 136
BASE = 32


def flip(me, i, shards):
    out, bit = 0, 1
    while bit < shards:
        out = out + lax.rem(lax.div(me, bit) + lax.div(i, bit), 2) * bit
        bit *= 2
    return out


def matmul(a, b):
    return lax.dot_general(a, b, (((1,), (0,)), ((), ())), preferred_element_type=jnp.float32)


def matmul_nt(a, b):
    return lax.dot_general(a, b, (((1,), (1,)), ((), ())), preferred_element_type=jnp.float32)


def circle(rows, columns, length):
    angles = 2.0 * math.pi / length * lax.rem(rows * columns, length).astype(jnp.float32)
    return jnp.cos(angles), jnp.sin(angles)


def fill(count, width, row_at, column_at, length, write):
    row = lax.broadcasted_iota(jnp.int32, (BASE, width), 0) + row_at
    column = lax.broadcasted_iota(jnp.int32, (BASE, width), 1) + column_at
    cos, sin = circle(row, column, length)
    line = lax.broadcasted_iota(jnp.int32, (1, width), 1) + column_at

    def step(i, carry):
        turn_cos, turn_sin = circle(i * BASE, line, length)
        here = pl.ds(pl.multiple_of(i * BASE, BASE), BASE)
        write(here, i, cos * turn_cos - sin * turn_sin, sin * turn_cos + cos * turn_sin)
        return carry

    lax.fori_loop(0, count // BASE, step, 0)


def convolve(signal, filt, ext, shards):
    a_loc, inner, channels = signal.shape
    d_loc, n_outer = filt.shape[1:3]
    ch_loc = channels // shards
    half = shards // 2
    d_half = half * d_loc
    f_ch = half * ch_loc
    step = 256
    chunks = n_outer // step
    groups = a_loc // GROUP
    rest = a_loc - GROUP
    d_group = min(GROUP, d_loc)
    inner_scale = 1.0 / math.sqrt(inner)
    outer_scale = 1.0 / math.sqrt(n_outer)
    ahead = min(4, ch_loc)

    def kernel(
        sig_ref, filt_ref, ext_ref, conv_ref, filt_t,
        s_buf, f_buf, e_buf, sig_t, outer_t, fwd_t, inv_t, tcb, tbc, r_buf, o_buf,
        l_buf, f_stage, turn,
        first_send, first_recv, sig_send, sig_recv, filt_send, filt_recv, ext_send, ext_recv,
        out_send, out_recv, load_sem, stage_sem,
    ):
        me = lax.axis_index("seq")
        side = lax.div(me, half)
        mine = lax.rem(me, half)
        barrier = pltpu.get_barrier_semaphore()

        def load_signal(g):
            return pltpu.make_async_copy(
                sig_ref.at[pl.ds(g * GROUP, GROUP)], l_buf.at[g % 2], load_sem.at[g % 2]
            )

        pieces = [
            (p, d, c)
            for p in range(2)
            for d in range(d_loc // d_group)
            for c in range(n_outer // inner)
        ]

        def load_filter(n):
            p, d, c = pieces[n]
            slot = (groups + n) % 2
            return pltpu.make_async_copy(
                filt_ref.at[p, pl.ds(d * d_group, d_group), pl.ds(c * inner, inner)],
                l_buf.at[slot, pl.ds(0, d_group)],
                load_sem.at[slot],
            )

        loads = [(load_signal, g) for g in range(groups)]
        loads += [(load_filter, n) for n in range(len(pieces))]

        def prefetch(n):
            if n < len(loads):
                make, at = loads[n]
                make(at).start()

        prefetch(0)
        prefetch(1)

        def greet(i, carry):
            pl.semaphore_signal(
                barrier, inc=1, device_id={"seq": lax.rem(me + i, shards)}, device_id_type=MESH
            )
            return carry

        lax.fori_loop(1, shards, greet, 0)

        def to_channels(slot, rows, first, count, store):
            def columns(j, carry):
                lanes = pl.ds(pl.multiple_of(j * LANES, LANES), LANES)
                for r in range(rows):
                    tile = l_buf[slot, r, lanes, :].astype(jnp.float32)
                    turn[pl.ds(r, channels, stride=PITCH), :] = tile.T

                def each(i, carry):
                    for n in range(8):
                        at = pl.multiple_of((first + i * 8 + n) * PITCH, 8)
                        store(i * 8 + n, lanes, turn[pl.ds(at, rows), :].astype(jnp.bfloat16))
                    return carry

                lax.fori_loop(0, count // 8, each, 0)
                return carry

            lax.fori_loop(0, inner // LANES, columns, 0)

        def turn_signal(g):
            load_signal(g).wait()

            def store(ch, lanes, tile):
                sig_t[ch, g * GROUP : (g + 1) * GROUP, lanes] = tile

            to_channels(g % 2, GROUP, 0, channels, store)
            prefetch(g + 2)

        def rows(s, skip, size):
            return pl.ds(pl.multiple_of(s * a_loc + skip, GROUP), size)

        def own(s):
            return pl.ds(pl.multiple_of(s * ch_loc, ch_loc), ch_loc)

        top = pl.ds(0, GROUP)
        below = pl.ds(GROUP, rest)
        turn_signal(0)
        pl.semaphore_wait(barrier, shards - 1)

        def send_first(i, carry):
            to = flip(me, shards - i, shards)
            pltpu.make_async_remote_copy(
                src_ref=sig_t.at[own(to), top],
                dst_ref=s_buf.at[:, rows(me, 0, GROUP)],
                send_sem=first_send,
                recv_sem=first_recv,
                device_id={"seq": to},
                device_id_type=MESH,
            ).start()
            return carry

        lax.fori_loop(1, shards, send_first, 0)
        pltpu.make_async_copy(
            sig_t.at[own(me), top], s_buf.at[:, rows(me, 0, GROUP)], first_recv
        ).start()

        @pl.when(mine == 0)
        def _():
            def send_ext(i, carry):
                to = (1 - side) * half + i
                pltpu.make_async_remote_copy(
                    src_ref=ext_ref.at[to],
                    dst_ref=e_buf,
                    send_sem=ext_send,
                    recv_sem=ext_recv,
                    device_id={"seq": to},
                    device_id_type=MESH,
                ).start()
                return carry

            lax.fori_loop(0, half, send_ext, 0)

        def send_signal(k):
            if rest == 0:
                return

            def send(i, carry):
                to = flip(me, shards - i, shards)
                pltpu.make_async_remote_copy(
                    src_ref=sig_t.at[to * ch_loc + k, below],
                    dst_ref=s_buf.at[k, rows(me, GROUP, rest)],
                    send_sem=sig_send.at[k],
                    recv_sem=sig_recv.at[k],
                    device_id={"seq": to},
                    device_id_type=MESH,
                ).start()
                return carry

            lax.fori_loop(1, shards, send, 0)
            pltpu.make_async_copy(
                sig_t.at[me * ch_loc + k, below], s_buf.at[k, rows(me, GROUP, rest)], sig_recv.at[k]
            ).start()

        def send_filter(k):
            def send(i, carry):
                to = flip(me, half - i, shards)
                pltpu.make_async_remote_copy(
                    src_ref=filt_t.at[lax.rem(to, half) * ch_loc + k],
                    dst_ref=f_buf.at[k, :, mine],
                    send_sem=filt_send.at[k],
                    recv_sem=filt_recv.at[k],
                    device_id={"seq": to},
                    device_id_type=MESH,
                ).start()
                return carry

            lax.fori_loop(1, half, send, 0)
            pltpu.make_async_copy(
                filt_t.at[mine * ch_loc + k], f_buf.at[k, :, mine], filt_recv.at[k]
            ).start()

        for g in range(1, groups):
            turn_signal(g)
        for k in range(ahead):
            send_signal(k)

        def stage(n):
            p, d, c = pieces[n]
            return pltpu.make_async_copy(
                f_stage.at[n % 2],
                filt_t.at[:, p, pl.ds(d * d_group, d_group), pl.ds(c * inner, inner)],
                stage_sem.at[n % 2],
            )

        for n in range(len(pieces)):
            load_filter(n).wait()
            if n >= 2:
                stage(n - 2).wait()

            def store(ch, lanes, tile):
                f_stage[n % 2, ch, :, lanes] = tile

            to_channels((groups + n) % 2, d_group, side * f_ch, f_ch, store)
            prefetch(groups + n + 2)
            stage(n).start()
        for n in range(max(len(pieces) - 2, 0), len(pieces)):
            stage(n).wait()
        for k in range(ahead):
            send_filter(k)

        def write_outer(here, i, cos, sin):
            outer_t[here, :] = cos.astype(jnp.bfloat16)
            low = pl.ds(pl.multiple_of(n_outer + i * BASE, BASE), BASE)
            outer_t[low, :] = (-sin).astype(jnp.bfloat16)

        def write_fwd(here, i, cos, sin):
            low = pl.ds(pl.multiple_of(d_half + i * BASE, BASE), BASE)
            fwd_t[here, 0:inner] = cos.astype(jnp.bfloat16)
            fwd_t[here, inner:] = sin.astype(jnp.bfloat16)
            fwd_t[low, 0:inner] = (-sin).astype(jnp.bfloat16)
            fwd_t[low, inner:] = cos.astype(jnp.bfloat16)

        def write_inv(here, i, cos, sin):
            low = pl.ds(pl.multiple_of(inner + i * BASE, BASE), BASE)
            inv_t[here, 0:d_half] = cos.astype(jnp.bfloat16)
            inv_t[here, d_half:] = (-sin).astype(jnp.bfloat16)
            inv_t[low, 0:d_half] = sin.astype(jnp.bfloat16)
            inv_t[low, d_half:] = cos.astype(jnp.bfloat16)

        def write_cb(here, i, cos, sin):
            tcb[0, here, :] = cos * outer_scale
            tcb[1, here, :] = sin * outer_scale

        def write_bc(here, i, cos, sin):
            tbc[0, here, :] = cos * inner_scale
            tbc[1, here, :] = sin * inner_scale

        length = n_outer * inner
        fill(n_outer, n_outer, 0, 0, n_outer, write_outer)
        fill(n_outer, inner, 0, 0, length, write_cb)
        fill(d_half, inner, side * d_half, 0, inner, write_fwd)
        fill(inner, d_half, 0, side * d_half, inner, write_inv)
        fill(inner, n_outer, 0, 0, length, write_bc)

        everything = s_buf.at[:, pl.ds(0, shards * GROUP)]
        pltpu.make_async_copy(everything, everything, first_recv).wait()
        pltpu.make_async_copy(e_buf, e_buf, ext_recv).wait()

        b_row = lax.broadcasted_iota(jnp.int32, (1, inner), 1)
        b_col = lax.broadcasted_iota(jnp.int32, (inner, 1), 0)
        swing = (1 - side).astype(jnp.float32)
        sign_row = 1.0 - 2.0 * swing * (b_row % 2).astype(jnp.float32)
        sign_col = 1.0 - 2.0 * swing * (b_col % 2).astype(jnp.float32)

        def channel(k, carry):
            slot = lax.rem(k, 2)

            @pl.when(k + ahead < ch_loc)
            def _():
                send_signal(k + ahead)
                send_filter(k + ahead)

            if rest:
                part = s_buf.at[k, pl.ds(0, shards * rest)]
                pltpu.make_async_copy(part, part, sig_recv.at[k]).wait()
            pltpu.make_async_copy(f_buf.at[k], f_buf.at[k], filt_recv.at[k]).wait()
            special = e_buf[k, :, 0:1]

            def forward(j, carry):
                at = pl.multiple_of(j * step, step)
                here = pl.ds(at, step)
                x = s_buf[k]
                f_re = matmul(outer_t[here, :], x)
                f_im = matmul(outer_t[pl.ds(pl.multiple_of(n_outer + at, step), step), :], x)
                cos, sin = tcb[0, here, :], tcb[1, here, :]
                q_re = (f_re * cos + f_im * sin).astype(jnp.bfloat16)
                q_im = (f_im * cos - f_re * sin).astype(jnp.bfloat16)
                q = jnp.concatenate([q_re, q_im], axis=1)
                spectrum = matmul_nt(fwd_t[...], q) * inner_scale
                spectrum = spectrum.astype(jnp.bfloat16).astype(jnp.float32)
                s_re, s_im = spectrum[:d_half], spectrum[d_half:]
                h_re = f_buf[k, 0, :, :, here].astype(jnp.float32).reshape(d_half, step)
                h_im = f_buf[k, 1, :, :, here].astype(jnp.float32).reshape(d_half, step)
                d_at = lax.broadcasted_iota(jnp.int32, (d_half, step), 0)
                c_at = lax.broadcasted_iota(jnp.int32, (d_half, step), 1) + at
                share = jnp.where((d_at == 0) & (c_at == 0), 0.5, 1.0)
                product = jnp.concatenate(
                    [(s_re * h_re - s_im * h_im) * share, (s_re * h_im + s_im * h_re) * share],
                    axis=0,
                ).astype(jnp.bfloat16)
                edge = jnp.sum(q_re[0:1].astype(jnp.float32) * sign_row, axis=1, keepdims=True)
                edge = (edge * inner_scale).astype(jnp.bfloat16).astype(jnp.float32)
                edge = (edge * special).astype(jnp.bfloat16).astype(jnp.float32) * 0.5
                c_row = lax.broadcasted_iota(jnp.int32, (1, step), 1) + at
                edge = jnp.where(c_row == 0, edge, 0.0)
                u = matmul(inv_t[...], product)
                u_re, u_im = u[:inner] + sign_col * edge, u[inner:]
                cos, sin = tbc[0, :, here], tbc[1, :, here]
                r_buf[0, :, here] = (u_re * cos - u_im * sin).astype(jnp.bfloat16)
                r_buf[1, :, here] = (u_re * sin + u_im * cos).astype(jnp.bfloat16)
                return carry

            lax.fori_loop(0, chunks, forward, 0)

            @pl.when(k >= 2)
            def _():
                pltpu.make_async_copy(o_buf.at[slot], o_buf.at[slot], out_send.at[slot]).wait()

            def backward(j, carry):
                at = pl.multiple_of(j * step, step)
                conv = matmul_nt(outer_t[pl.ds(at, step), :], r_buf[0]) + matmul_nt(
                    outer_t[pl.ds(pl.multiple_of(n_outer + at, step), step), :], r_buf[1]
                )
                conv = conv * (2.0 * outer_scale)
                o_buf[slot, pl.ds(at, step), :] = conv.astype(jnp.bfloat16)
                return carry

            lax.fori_loop(0, chunks, backward, 0)
            pltpu.make_async_copy(
                o_buf.at[slot, rows(me, 0, a_loc)], conv_ref.at[me, k], out_send.at[slot]
            ).start()

            def send_out(i, carry):
                to = flip(me, shards - i, shards)
                pltpu.make_async_remote_copy(
                    src_ref=o_buf.at[slot, rows(to, 0, a_loc)],
                    dst_ref=conv_ref.at[me, k],
                    send_sem=out_send.at[slot],
                    recv_sem=out_recv,
                    device_id={"seq": to},
                    device_id_type=MESH,
                ).start()
                return carry

            lax.fori_loop(1, shards, send_out, 0)
            return carry

        lax.fori_loop(0, ch_loc, channel, 0)
        for slot in range(min(2, ch_loc)):
            pltpu.make_async_copy(o_buf.at[slot], o_buf.at[slot], out_send.at[slot]).wait()
        sent = sig_t.at[pl.ds(0, (shards - 1) * ch_loc), top]
        pltpu.make_async_copy(sent, sent, first_send).wait()
        for k in range(ch_loc):
            if rest:
                sent = sig_t.at[pl.ds(0, shards - 1), pl.ds(0, rest)]
                pltpu.make_async_copy(sent, sent, sig_send.at[k]).wait()
            sent = filt_t.at[pl.ds(0, half - 1)]
            pltpu.make_async_copy(sent, sent, filt_send.at[k]).wait()

        @pl.when(mine == 0)
        def _():
            sent = ext_ref.at[pl.ds(0, half)]
            pltpu.make_async_copy(sent, sent, ext_send).wait()

        others = conv_ref.at[pl.ds(0, shards - 1)]
        pltpu.make_async_copy(others, others, out_recv).wait()

    anywhere = pl.BlockSpec(memory_space=pl.ANY)
    bf16, f32 = jnp.bfloat16, jnp.float32
    per_channel = pltpu.SemaphoreType.DMA((ch_loc,))
    single = pltpu.SemaphoreType.DMA
    pair = pltpu.SemaphoreType.DMA((2,))
    return pl.pallas_call(
        kernel,
        out_shape=(
            jax.ShapeDtypeStruct((shards, ch_loc, a_loc, inner), bf16),
            jax.ShapeDtypeStruct((f_ch, 2, d_loc, n_outer), bf16),
        ),
        in_specs=[anywhere] * 3,
        out_specs=(anywhere, anywhere),
        scratch_shapes=[
            pltpu.VMEM((ch_loc, n_outer, inner), bf16),
            pltpu.VMEM((ch_loc, 2, half, d_loc, n_outer), bf16),
            pltpu.VMEM(ext.shape[1:], f32),
            pltpu.VMEM((channels, a_loc, inner), bf16),
            pltpu.VMEM((2 * n_outer, n_outer), bf16),
            pltpu.VMEM((2 * d_half, 2 * inner), bf16),
            pltpu.VMEM((2 * inner, 2 * d_half), bf16),
            pltpu.VMEM((2, n_outer, inner), f32),
            pltpu.VMEM((2, inner, n_outer), f32),
            pltpu.VMEM((2, inner, n_outer), bf16),
            pltpu.VMEM((2, n_outer, inner), bf16),
            pltpu.VMEM((2, GROUP, inner, channels), bf16),
            pltpu.VMEM((2, f_ch, d_group, inner), bf16),
            pltpu.VMEM((channels * PITCH, LANES), f32),
            single,
            single,
            per_channel,
            per_channel,
            per_channel,
            per_channel,
            single,
            single,
            pair,
            single,
            pair,
            pair,
        ],
        compiler_params=pltpu.CompilerParams(
            collective_id=0, has_side_effects=True, vmem_limit_bytes=67043328
        ),
        name="convolve",
    )(signal, filt, ext)[0]


def finish(convolved, signal, gate, skip):
    a_loc, inner, channels = signal.shape

    def kernel(conv_ref, sig_ref, gate_ref, skip_ref, out_ref, turn):
        def each(i, carry):
            for n in range(8):
                ch = i * 8 + n
                turn[pl.ds(ch, GROUP, stride=STRIDE), :] = conv_ref[ch].astype(jnp.float32)
            return carry

        lax.fori_loop(0, channels // 8, each, 0)
        for a in range(GROUP):
            conv = turn[a * STRIDE : a * STRIDE + channels, :].T
            full = conv + skip_ref[...] * sig_ref[a].astype(jnp.float32)
            out_ref[a] = (gate_ref[a].astype(jnp.float32) * full).astype(jnp.bfloat16)

    flat = pl.BlockSpec((GROUP, LANES, channels), lambda i, j: (i, j, 0))
    return pl.pallas_call(
        kernel,
        out_shape=jax.ShapeDtypeStruct(signal.shape, jnp.bfloat16),
        grid=(a_loc // GROUP, inner // LANES),
        in_specs=[
            pl.BlockSpec((channels, GROUP, LANES), lambda i, j: (0, i, j)),
            flat,
            flat,
            pl.BlockSpec((1, channels), lambda i, j: (0, 0)),
        ],
        out_specs=flat,
        scratch_shapes=[pltpu.VMEM((GROUP * STRIDE, LANES), jnp.float32)],
        name="finish",
    )(convolved.reshape(channels, a_loc, inner), signal, gate, skip)


def local(signal, gate_values, skip_gain, filter_spectrum):
    shards = lax.axis_size("seq")
    positions, channels = signal.shape
    d_loc, n_outer = filter_spectrum.shape[1:3]
    grid = (n_outer // shards, d_loc * shards, channels)
    ch_loc = channels // shards
    ext = jnp.broadcast_to(
        filter_spectrum[0, 0, 0].astype(jnp.float32).reshape(shards, ch_loc, 1, 1),
        (shards, ch_loc, 1, LANES),
    )
    convolved = convolve(signal.reshape(grid), filter_spectrum, ext, shards)
    result = finish(
        convolved, signal.reshape(grid), gate_values.reshape(grid), skip_gain.reshape(1, channels)
    )
    return result.reshape(positions, channels)


def solution(mesh):
    return jax.shard_map(
        local,
        mesh=mesh,
        in_specs=(P("seq", "chan"), P("seq", "chan"), P("chan"), P(None, "seq", None, "chan")),
        out_specs=P("seq", "chan"),
        check_vma=False,
    )
```

```python
import math

import jax
import jax.numpy as jnp
from jax import lax
from jax.experimental import pallas as pl
from jax.experimental.pallas import tpu as pltpu
from jax.sharding import PartitionSpec as P

MESH = pl.DeviceIdType.MESH
LANES = 128
GROUP = 16
PITCH = 24
STRIDE = 136
BASE = 32


def flip(me, i, shards):
    out, bit = 0, 1
    while bit < shards:
        out = out + lax.rem(lax.div(me, bit) + lax.div(i, bit), 2) * bit
        bit *= 2
    return out


def matmul(a, b):
    return lax.dot_general(a, b, (((1,), (0,)), ((), ())), preferred_element_type=jnp.float32)


def matmul_nt(a, b):
    return lax.dot_general(a, b, (((1,), (1,)), ((), ())), preferred_element_type=jnp.float32)


def circle(rows, columns, length):
    angles = 2.0 * math.pi / length * lax.rem(rows * columns, length).astype(jnp.float32)
    return jnp.cos(angles), jnp.sin(angles)


def fill(count, width, row_at, column_at, length, write):
    row = lax.broadcasted_iota(jnp.int32, (BASE, width), 0) + row_at
    column = lax.broadcasted_iota(jnp.int32, (BASE, width), 1) + column_at
    cos, sin = circle(row, column, length)
    line = lax.broadcasted_iota(jnp.int32, (1, width), 1) + column_at

    def step(i, carry):
        turn_cos, turn_sin = circle(i * BASE, line, length)
        here = pl.ds(pl.multiple_of(i * BASE, BASE), BASE)
        write(here, i, cos * turn_cos - sin * turn_sin, sin * turn_cos + cos * turn_sin)
        return carry

    lax.fori_loop(0, count // BASE, step, 0)


def to_positions(turn, shards, ch_loc, load, store):
    channels = shards * ch_loc

    def each(t, carry):
        for k in range(ch_loc):
            at = t * ch_loc + k
            turn[pl.ds(at, GROUP, stride=STRIDE), :] = load(t, k).astype(jnp.float32)
        return carry

    lax.fori_loop(0, shards, each, 0)
    for a in range(GROUP):
        store(a, turn[a * STRIDE : a * STRIDE + channels, :].T)


def convolve(signal, gate, skip, filt, ext, shards):
    a_loc, inner, channels = signal.shape
    d_loc, n_outer = filt.shape[1:3]
    ch_loc = channels // shards
    half = shards // 2
    d_half = half * d_loc
    f_ch = half * ch_loc
    step = 256
    chunks = n_outer // step
    groups = a_loc // GROUP
    rest = a_loc - GROUP
    d_group = min(GROUP, d_loc)
    inner_scale = 1.0 / math.sqrt(inner)
    outer_scale = 1.0 / math.sqrt(n_outer)
    ahead = min(2, ch_loc)

    def kernel(
        sig_ref, gate_ref, skip_ref, filt_ref, ext_ref, conv_ref, filt_t, part_ref,
        s_buf, f_buf, e_buf, sig_t, outer_t, fwd_t, inv_t, tcb, tbc, r_buf, o_buf,
        l_buf, f_stage, turn, c_buf,
        first_send, first_recv, sig_send, sig_recv, filt_send, filt_recv, ext_send, ext_recv,
        out_send, out_own, out_recv, end_recv, load_sem, stage_sem, tail_sem, part_sem,
    ):
        me = lax.axis_index("seq")
        side = lax.div(me, half)
        mine = lax.rem(me, half)
        barrier = pltpu.get_barrier_semaphore()

        def load_signal(g):
            return pltpu.make_async_copy(
                sig_ref.at[pl.ds(g * GROUP, GROUP)], l_buf.at[g % 2], load_sem.at[g % 2]
            )

        pieces = [
            (p, d, c)
            for p in range(2)
            for d in range(d_loc // d_group)
            for c in range(n_outer // inner)
        ]

        def load_filter(n):
            p, d, c = pieces[n]
            slot = (groups + n) % 2
            return pltpu.make_async_copy(
                filt_ref.at[p, pl.ds(d * d_group, d_group), pl.ds(c * inner, inner)],
                l_buf.at[slot, pl.ds(0, d_group)],
                load_sem.at[slot],
            )

        loads = [(load_signal, g) for g in range(groups)]
        loads += [(load_filter, n) for n in range(len(pieces))]

        def prefetch(n):
            if n < len(loads):
                make, at = loads[n]
                make(at).start()

        prefetch(0)
        prefetch(1)

        def greet(i, carry):
            pl.semaphore_signal(
                barrier, inc=1, device_id={"seq": lax.rem(me + i, shards)}, device_id_type=MESH
            )
            return carry

        lax.fori_loop(1, shards, greet, 0)

        def to_channels(slot, rows, first, count, store):
            def columns(j, carry):
                lanes = pl.ds(pl.multiple_of(j * LANES, LANES), LANES)
                for r in range(rows):
                    tile = l_buf[slot, r, lanes, :].astype(jnp.float32)
                    turn[pl.ds(r, channels, stride=PITCH), :] = tile.T

                def each(i, carry):
                    for n in range(8):
                        at = pl.multiple_of((first + i * 8 + n) * PITCH, 8)
                        store(i * 8 + n, lanes, turn[pl.ds(at, rows), :].astype(jnp.bfloat16))
                    return carry

                lax.fori_loop(0, count // 8, each, 0)
                return carry

            lax.fori_loop(0, inner // LANES, columns, 0)

        def turn_signal(g):
            load_signal(g).wait()

            def store(ch, lanes, tile):
                sig_t[ch, g * GROUP : (g + 1) * GROUP, lanes] = tile

            to_channels(g % 2, GROUP, 0, channels, store)
            prefetch(g + 2)

        def rows(s, skip, size):
            return pl.ds(pl.multiple_of(s * a_loc + skip, GROUP), size)

        def group_rows(g):
            return pl.ds(pl.multiple_of(g * GROUP, GROUP), GROUP)

        def own(s):
            return pl.ds(pl.multiple_of(s * ch_loc, ch_loc), ch_loc)

        top = pl.ds(0, GROUP)
        below = pl.ds(GROUP, rest)
        turn_signal(0)
        pl.semaphore_wait(barrier, shards - 1)

        parity = lax.rem(me, 2)

        def send_first(i, carry):
            to = flip(me, (1 - parity) * (shards - i) + parity * i, shards)
            pltpu.make_async_remote_copy(
                src_ref=sig_t.at[own(to), top],
                dst_ref=s_buf.at[:, rows(me, 0, GROUP)],
                send_sem=first_send,
                recv_sem=first_recv,
                device_id={"seq": to},
                device_id_type=MESH,
            ).start()
            return carry

        lax.fori_loop(1, shards, send_first, 0)
        pltpu.make_async_copy(
            sig_t.at[own(me), top], s_buf.at[:, rows(me, 0, GROUP)], first_recv
        ).start()

        @pl.when(mine == 0)
        def _():
            def send_ext(i, carry):
                to = (1 - side) * half + i
                pltpu.make_async_remote_copy(
                    src_ref=ext_ref.at[to],
                    dst_ref=e_buf,
                    send_sem=ext_send,
                    recv_sem=ext_recv,
                    device_id={"seq": to},
                    device_id_type=MESH,
                ).start()
                return carry

            lax.fori_loop(0, half, send_ext, 0)

        quarter = half // 2

        def ordered(far, near, middle=None):
            def far_loop():
                def one(n, carry):
                    far(half + (1 - lax.rem(n, 2)) * quarter + lax.div(n, 2))
                    return carry

                lax.fori_loop(0, half, one, 0)

            def near_loop(send, low, high):
                def one(i, carry):
                    send(i)
                    return carry

                lax.fori_loop(low, high, one, 0)

            pl.when(parity == 0)(far_loop)
            for low, high in ((quarter, half), (1, quarter)):
                if middle is not None:
                    near_loop(middle, low, high)
                near_loop(near, low, high)
            pl.when(parity == 1)(far_loop)

        def send_round(k):
            def send_signal(i):
                to = flip(me, i, shards)
                pltpu.make_async_remote_copy(
                    src_ref=sig_t.at[to * ch_loc + k, below],
                    dst_ref=s_buf.at[k, rows(me, GROUP, rest)],
                    send_sem=sig_send.at[k],
                    recv_sem=sig_recv.at[k],
                    device_id={"seq": to},
                    device_id_type=MESH,
                ).start()

            def send_filter(i):
                to = flip(me, i, shards)
                pltpu.make_async_remote_copy(
                    src_ref=filt_t.at[lax.rem(to, half) * ch_loc + k],
                    dst_ref=f_buf.at[k, :, mine],
                    send_sem=filt_send.at[k],
                    recv_sem=filt_recv.at[k],
                    device_id={"seq": to},
                    device_id_type=MESH,
                ).start()

            def nothing(i):
                return None

            signal_step = send_signal if rest else nothing
            ordered(signal_step, signal_step, send_filter)
            if rest:
                pltpu.make_async_copy(
                    sig_t.at[me * ch_loc + k, below],
                    s_buf.at[k, rows(me, GROUP, rest)],
                    sig_recv.at[k],
                ).start()
            pltpu.make_async_copy(
                filt_t.at[mine * ch_loc + k], f_buf.at[k, :, mine], filt_recv.at[k]
            ).start()

        for g in range(1, groups):
            turn_signal(g)
        def stage(n):
            p, d, c = pieces[n]
            return pltpu.make_async_copy(
                f_stage.at[n % 2],
                filt_t.at[:, p, pl.ds(d * d_group, d_group), pl.ds(c * inner, inner)],
                stage_sem.at[n % 2],
            )

        for n in range(len(pieces)):
            load_filter(n).wait()
            if n >= 2:
                stage(n - 2).wait()

            def store(ch, lanes, tile):
                f_stage[n % 2, ch, :, lanes] = tile

            to_channels((groups + n) % 2, d_group, side * f_ch, f_ch, store)
            prefetch(groups + n + 2)
            stage(n).start()
        for n in range(max(len(pieces) - 2, 0), len(pieces)):
            stage(n).wait()
        for k in range(ahead):
            send_round(k)

        def write_outer(here, i, cos, sin):
            outer_t[here, :] = cos.astype(jnp.bfloat16)
            low = pl.ds(pl.multiple_of(n_outer + i * BASE, BASE), BASE)
            outer_t[low, :] = (-sin).astype(jnp.bfloat16)

        def write_fwd(here, i, cos, sin):
            low = pl.ds(pl.multiple_of(d_half + i * BASE, BASE), BASE)
            fwd_t[here, 0:inner] = cos.astype(jnp.bfloat16)
            fwd_t[here, inner:] = sin.astype(jnp.bfloat16)
            fwd_t[low, 0:inner] = (-sin).astype(jnp.bfloat16)
            fwd_t[low, inner:] = cos.astype(jnp.bfloat16)

        def write_inv(here, i, cos, sin):
            low = pl.ds(pl.multiple_of(inner + i * BASE, BASE), BASE)
            inv_t[here, 0:d_half] = cos.astype(jnp.bfloat16)
            inv_t[here, d_half:] = (-sin).astype(jnp.bfloat16)
            inv_t[low, 0:d_half] = sin.astype(jnp.bfloat16)
            inv_t[low, d_half:] = cos.astype(jnp.bfloat16)

        def write_cb(here, i, cos, sin):
            tcb[0, here, :] = cos * outer_scale
            tcb[1, here, :] = sin * outer_scale

        def write_bc(here, i, cos, sin):
            tbc[0, here, :] = cos * inner_scale
            tbc[1, here, :] = sin * inner_scale

        length = n_outer * inner
        fill(n_outer, n_outer, 0, 0, n_outer, write_outer)
        fill(n_outer, inner, 0, 0, length, write_cb)
        fill(d_half, inner, side * d_half, 0, inner, write_fwd)
        fill(inner, d_half, 0, side * d_half, inner, write_inv)
        fill(inner, n_outer, 0, 0, length, write_bc)

        everything = s_buf.at[:, pl.ds(0, shards * GROUP)]
        pltpu.make_async_copy(everything, everything, first_recv).wait()
        pltpu.make_async_copy(e_buf, e_buf, ext_recv).wait()

        b_row = lax.broadcasted_iota(jnp.int32, (1, inner), 1)
        b_col = lax.broadcasted_iota(jnp.int32, (inner, 1), 0)
        swing = (1 - side).astype(jnp.float32)
        sign_row = 1.0 - 2.0 * swing * (b_row % 2).astype(jnp.float32)
        sign_col = 1.0 - 2.0 * swing * (b_col % 2).astype(jnp.float32)

        def channel(k, carry):
            slot = lax.rem(k, 2)

            if rest:
                part = s_buf.at[k, pl.ds(0, shards * rest)]
                pltpu.make_async_copy(part, part, sig_recv.at[k]).wait()
            pltpu.make_async_copy(f_buf.at[k], f_buf.at[k], filt_recv.at[k]).wait()
            special = e_buf[k, :, 0:1]

            @pl.when(k + ahead < ch_loc)
            def _():
                send_round(k + ahead)


            def forward(j, carry):
                at = pl.multiple_of(j * step, step)
                here = pl.ds(at, step)
                x = s_buf[k]
                f_re = matmul(outer_t[here, :], x)
                f_im = matmul(outer_t[pl.ds(pl.multiple_of(n_outer + at, step), step), :], x)
                cos, sin = tcb[0, here, :], tcb[1, here, :]
                q_re = (f_re * cos + f_im * sin).astype(jnp.bfloat16)
                q_im = (f_im * cos - f_re * sin).astype(jnp.bfloat16)
                q = jnp.concatenate([q_re, q_im], axis=1)
                spectrum = matmul_nt(fwd_t[...], q) * inner_scale
                spectrum = spectrum.astype(jnp.bfloat16).astype(jnp.float32)
                s_re, s_im = spectrum[:d_half], spectrum[d_half:]
                h_re = f_buf[k, 0, :, :, here].astype(jnp.float32).reshape(d_half, step)
                h_im = f_buf[k, 1, :, :, here].astype(jnp.float32).reshape(d_half, step)
                d_at = lax.broadcasted_iota(jnp.int32, (d_half, step), 0)
                c_at = lax.broadcasted_iota(jnp.int32, (d_half, step), 1) + at
                share = jnp.where((d_at == 0) & (c_at == 0), 0.5, 1.0)
                product = jnp.concatenate(
                    [(s_re * h_re - s_im * h_im) * share, (s_re * h_im + s_im * h_re) * share],
                    axis=0,
                ).astype(jnp.bfloat16)
                edge = jnp.sum(q_re[0:1].astype(jnp.float32) * sign_row, axis=1, keepdims=True)
                edge = (edge * inner_scale).astype(jnp.bfloat16).astype(jnp.float32)
                edge = (edge * special).astype(jnp.bfloat16).astype(jnp.float32) * 0.5
                c_row = lax.broadcasted_iota(jnp.int32, (1, step), 1) + at
                edge = jnp.where(c_row == 0, edge, 0.0)
                u = matmul(inv_t[...], product)
                u_re, u_im = u[:inner] + sign_col * edge, u[inner:]
                cos, sin = tbc[0, :, here], tbc[1, :, here]
                r_buf[0, :, here] = (u_re * cos - u_im * sin).astype(jnp.bfloat16)
                r_buf[1, :, here] = (u_re * sin + u_im * cos).astype(jnp.bfloat16)
                return carry

            lax.fori_loop(0, chunks, forward, 0)

            @pl.when(k >= 2)
            def _():
                sent = o_buf.at[slot, pl.ds(0, (shards - 1) * a_loc)]
                pltpu.make_async_copy(sent, sent, out_send.at[slot]).wait()
                kept = o_buf.at[slot, pl.ds(0, a_loc)]
                pltpu.make_async_copy(kept, kept, out_own.at[slot]).wait()

            def backward(j, carry):
                at = pl.multiple_of(j * step, step)
                conv = matmul_nt(outer_t[pl.ds(at, step), :], r_buf[0]) + matmul_nt(
                    outer_t[pl.ds(pl.multiple_of(n_outer + at, step), step), :], r_buf[1]
                )
                conv = conv * (2.0 * outer_scale)
                o_buf[slot, pl.ds(at, step), :] = conv.astype(jnp.bfloat16)
                return carry

            lax.fori_loop(0, chunks, backward, 0)
            pltpu.make_async_copy(
                o_buf.at[slot, rows(me, 0, a_loc)], conv_ref.at[me, k], out_own.at[slot]
            ).start()

            def send_out(i):
                to = flip(me, i, shards)
                pltpu.make_async_remote_copy(
                    src_ref=o_buf.at[slot, rows(to, 0, a_loc)],
                    dst_ref=conv_ref.at[me, k],
                    send_sem=out_send.at[slot],
                    recv_sem=out_recv,
                    device_id={"seq": to},
                    device_id_type=MESH,
                ).start()

            def send_end(g, carry):
                def send(i):
                    to = flip(me, i, shards)
                    pltpu.make_async_remote_copy(
                        src_ref=o_buf.at[slot, rows(to, g * GROUP, GROUP)],
                        dst_ref=conv_ref.at[me, k, group_rows(g)],
                        send_sem=out_send.at[slot],
                        recv_sem=end_recv.at[g],
                        device_id={"seq": to},
                        device_id_type=MESH,
                    ).start()

                ordered(send, send)
                return carry

            @pl.when(k < ch_loc - 1)
            def _():
                ordered(send_out, send_out)

            @pl.when(k == ch_loc - 1)
            def _():
                lax.fori_loop(0, groups, send_end, 0)

            return carry

        def tail_load(g):
            lane = 2 * (g % 2)
            return [
                pltpu.make_async_copy(ref.at[group_rows(g)], l_buf.at[lane + i], tail_sem.at[lane + i])
                for i, ref in enumerate((sig_ref, gate_ref))
            ]

        def tail_store(g):
            return pltpu.make_async_copy(
                l_buf.at[2 * (g % 2) + 1], part_ref.at[group_rows(g)], part_sem.at[g % 2]
            )

        for g in range(min(2, groups - 1)):
            for copy in tail_load(g):
                copy.start()
        lax.fori_loop(0, ch_loc, channel, 0)
        for k in range(max(ch_loc - 2, 0), ch_loc):
            kept = o_buf.at[k % 2, pl.ds(0, a_loc)]
            pltpu.make_async_copy(kept, kept, out_own.at[k % 2]).wait()
        if ch_loc > 1:
            others = conv_ref.at[pl.ds(0, shards - 1), pl.ds(0, ch_loc - 1)]
            pltpu.make_async_copy(others, others, out_recv).wait()

        for g in range(groups):
            landed = conv_ref.at[pl.ds(0, shards - 1), 0, pl.ds(0, GROUP)]
            pltpu.make_async_copy(landed, landed, end_recv.at[g]).wait()
            if g == groups - 1:
                break
            fetch = pltpu.make_async_copy(conv_ref.at[:, :, group_rows(g)], c_buf, tail_sem.at[4])
            fetch.start()
            for copy in tail_load(g):
                copy.wait()
            fetch.wait()
            lane = 2 * (g % 2)

            def columns(j, carry):
                lanes = pl.ds(pl.multiple_of(j * LANES, LANES), LANES)

                def load(t, k):
                    return c_buf[t, k, :, lanes]

                def store(a, conv):
                    full = conv + skip_ref[...] * l_buf[lane, a, lanes, :].astype(jnp.float32)
                    full = l_buf[lane + 1, a, lanes, :].astype(jnp.float32) * full
                    l_buf[lane + 1, a, lanes, :] = full.astype(jnp.bfloat16)

                to_positions(turn, shards, ch_loc, load, store)
                return carry

            lax.fori_loop(0, inner // LANES, columns, 0)
            tail_store(g).start()
            if g + 2 < groups - 1:
                tail_store(g).wait()
                for copy in tail_load(g + 2):
                    copy.start()
        for g in range(max(groups - 3, 0), groups - 1):
            tail_store(g).wait()
        for k in range(max(ch_loc - 2, 0), ch_loc):
            sent = o_buf.at[k % 2, pl.ds(0, (shards - 1) * a_loc)]
            pltpu.make_async_copy(sent, sent, out_send.at[k % 2]).wait()
        sent = sig_t.at[pl.ds(0, (shards - 1) * ch_loc), top]
        pltpu.make_async_copy(sent, sent, first_send).wait()
        for k in range(ch_loc):
            if rest:
                sent = sig_t.at[pl.ds(0, shards - 1), pl.ds(0, rest)]
                pltpu.make_async_copy(sent, sent, sig_send.at[k]).wait()
            sent = filt_t.at[pl.ds(0, half - 1)]
            pltpu.make_async_copy(sent, sent, filt_send.at[k]).wait()

        @pl.when(mine == 0)
        def _():
            sent = ext_ref.at[pl.ds(0, half)]
            pltpu.make_async_copy(sent, sent, ext_send).wait()

    anywhere = pl.BlockSpec(memory_space=pl.ANY)
    bf16, f32 = jnp.bfloat16, jnp.float32
    per_channel = pltpu.SemaphoreType.DMA((ch_loc,))
    single = pltpu.SemaphoreType.DMA
    pair = pltpu.SemaphoreType.DMA((2,))
    return pl.pallas_call(
        kernel,
        out_shape=(
            jax.ShapeDtypeStruct((shards, ch_loc, a_loc, inner), bf16),
            jax.ShapeDtypeStruct((f_ch, 2, d_loc, n_outer), bf16),
            jax.ShapeDtypeStruct((max(rest, GROUP), inner, channels), bf16),
        ),
        in_specs=[anywhere, anywhere, pl.BlockSpec(memory_space=pltpu.VMEM), anywhere, anywhere],
        out_specs=(anywhere, anywhere, anywhere),
        scratch_shapes=[
            pltpu.VMEM((ch_loc, n_outer, inner), bf16),
            pltpu.VMEM((ch_loc, 2, half, d_loc, n_outer), bf16),
            pltpu.VMEM(ext.shape[1:], f32),
            pltpu.VMEM((channels, a_loc, inner), bf16),
            pltpu.VMEM((2 * n_outer, n_outer), bf16),
            pltpu.VMEM((2 * d_half, 2 * inner), bf16),
            pltpu.VMEM((2 * inner, 2 * d_half), bf16),
            pltpu.VMEM((2, n_outer, inner), f32),
            pltpu.VMEM((2, inner, n_outer), f32),
            pltpu.VMEM((2, inner, n_outer), bf16),
            pltpu.VMEM((2, n_outer, inner), bf16),
            pltpu.VMEM((4, GROUP, inner, channels), bf16),
            pltpu.VMEM((2, f_ch, d_group, inner), bf16),
            pltpu.VMEM((channels * PITCH, LANES), f32),
            pltpu.VMEM((shards, ch_loc, GROUP, inner), bf16),
            single,
            single,
            per_channel,
            per_channel,
            per_channel,
            per_channel,
            single,
            single,
            pair,
            pair,
            single,
            pltpu.SemaphoreType.DMA((groups,)),
            pair,
            pair,
            pltpu.SemaphoreType.DMA((5,)),
            pair,
        ],
        compiler_params=pltpu.CompilerParams(
            collective_id=0, has_side_effects=True, vmem_limit_bytes=67043328
        ),
        name="convolve",
    )(signal, gate, skip, filt, ext)


def finish(convolved, part, signal, gate, skip):
    a_loc, inner, channels = signal.shape
    shards, ch_loc = convolved.shape[:2]
    done = a_loc - GROUP
    copies = done // GROUP
    chunks = inner // LANES

    def kernel(
        conv_ref, part_ref, sig_ref, gate_ref, skip_ref, out_ref,
        c_buf, s_buf, g_buf, p_buf, turn, in_sem, part_in, part_out, out_sem,
    ):
        last = pl.ds(done, GROUP)
        loads = [
            pltpu.make_async_copy(conv_ref.at[:, :, last], c_buf, in_sem.at[0]),
            pltpu.make_async_copy(sig_ref.at[last], s_buf, in_sem.at[1]),
            pltpu.make_async_copy(gate_ref.at[last], g_buf, in_sem.at[2]),
        ]
        moves = []
        for n in range(copies):
            rows = pl.ds(n * GROUP, GROUP)
            moves.append(
                (
                    pltpu.make_async_copy(part_ref.at[rows], p_buf.at[n], part_in.at[n]),
                    pltpu.make_async_copy(p_buf.at[n], out_ref.at[rows], part_out.at[n]),
                )
            )
        for copy in loads + [move[0] for move in moves]:
            copy.start()
        for copy in loads:
            copy.wait()
        stores = []
        for j in range(chunks):
            lanes = pl.ds(j * LANES, LANES)

            def load(t, k):
                return c_buf[t, k, :, lanes]

            def store(a, conv):
                full = conv + skip_ref[...] * s_buf[a, lanes, :].astype(jnp.float32)
                full = g_buf[a, lanes, :].astype(jnp.float32) * full
                g_buf[a, lanes, :] = full.astype(jnp.bfloat16)

            to_positions(turn, shards, ch_loc, load, store)
            stores.append(
                pltpu.make_async_copy(
                    g_buf.at[:, lanes], out_ref.at[last, lanes], out_sem.at[j]
                )
            )
            stores[-1].start()
            if j < copies:
                moves[j][0].wait()
                moves[j][1].start()
        for n in range(chunks, copies):
            moves[n][0].wait()
            moves[n][1].start()
        for copy in stores + [move[1] for move in moves]:
            copy.wait()

    anywhere = pl.BlockSpec(memory_space=pl.ANY)
    rows_shape = (GROUP, inner, channels)
    return pl.pallas_call(
        kernel,
        out_shape=jax.ShapeDtypeStruct(signal.shape, jnp.bfloat16),
        in_specs=[anywhere] * 4 + [pl.BlockSpec(memory_space=pltpu.VMEM)],
        out_specs=anywhere,
        scratch_shapes=[
            pltpu.VMEM((shards, ch_loc, GROUP, inner), jnp.bfloat16),
            pltpu.VMEM(rows_shape, jnp.bfloat16),
            pltpu.VMEM(rows_shape, jnp.bfloat16),
            pltpu.VMEM((max(copies, 1), *rows_shape), jnp.bfloat16),
            pltpu.VMEM((GROUP * STRIDE, LANES), jnp.float32),
            pltpu.SemaphoreType.DMA((3,)),
            pltpu.SemaphoreType.DMA((max(copies, 1),)),
            pltpu.SemaphoreType.DMA((max(copies, 1),)),
            pltpu.SemaphoreType.DMA((chunks,)),
        ],
        compiler_params=pltpu.CompilerParams(vmem_limit_bytes=67043328),
        name="finish",
    )(convolved, part, signal, gate, skip)


def local(signal, gate_values, skip_gain, filter_spectrum):
    shards = lax.axis_size("seq")
    positions, channels = signal.shape
    d_loc, n_outer = filter_spectrum.shape[1:3]
    grid = (n_outer // shards, d_loc * shards, channels)
    ch_loc = channels // shards
    ext = jnp.broadcast_to(
        filter_spectrum[0, 0, 0].astype(jnp.float32).reshape(shards, ch_loc, 1, 1),
        (shards, ch_loc, 1, LANES),
    )
    signal, gate = signal.reshape(grid), gate_values.reshape(grid)
    skip = skip_gain.reshape(1, channels)
    convolved, _, part = convolve(signal, gate, skip, filter_spectrum, ext, shards)
    result = finish(convolved, part, signal, gate, skip)
    return result.reshape(positions, channels)


def solution(mesh):
    return jax.shard_map(
        local,
        mesh=mesh,
        in_specs=(P("seq", "chan"), P("seq", "chan"), P("chan"), P(None, "seq", None, "chan")),
        out_specs=P("seq", "chan"),
        check_vma=False,
    )
```

```python
import math

import jax
import jax.numpy as jnp
from jax import lax
from jax.experimental import pallas as pl
from jax.experimental.pallas import tpu as pltpu
from jax.sharding import PartitionSpec as P

MESH = pl.DeviceIdType.MESH
LANES = 128
GROUP = 16
PITCH = 24
STRIDE = 136
BASE = 32


def flip(me, i, shards):
    out, bit = 0, 1
    while bit < shards:
        out = out + lax.rem(lax.div(me, bit) + lax.div(i, bit), 2) * bit
        bit *= 2
    return out


def matmul(a, b):
    return lax.dot_general(a, b, (((1,), (0,)), ((), ())), preferred_element_type=jnp.float32)


def matmul_nt(a, b):
    return lax.dot_general(a, b, (((1,), (1,)), ((), ())), preferred_element_type=jnp.float32)


def circle(rows, columns, length):
    angles = 2.0 * math.pi / length * lax.rem(rows * columns, length).astype(jnp.float32)
    return jnp.cos(angles), jnp.sin(angles)


def fill(count, width, row_at, column_at, length, write):
    row = lax.broadcasted_iota(jnp.int32, (BASE, width), 0) + row_at
    column = lax.broadcasted_iota(jnp.int32, (BASE, width), 1) + column_at
    cos, sin = circle(row, column, length)
    line = lax.broadcasted_iota(jnp.int32, (1, width), 1) + column_at

    def step(i, carry):
        turn_cos, turn_sin = circle(i * BASE, line, length)
        here = pl.ds(pl.multiple_of(i * BASE, BASE), BASE)
        write(here, i, cos * turn_cos - sin * turn_sin, sin * turn_cos + cos * turn_sin)
        return carry

    lax.fori_loop(0, count // BASE, step, 0)


def to_positions(turn, shards, ch_loc, load, store):
    channels = shards * ch_loc

    def each(t, carry):
        for k in range(ch_loc):
            at = t * ch_loc + k
            turn[pl.ds(at, GROUP, stride=STRIDE), :] = load(t, k).astype(jnp.float32)
        return carry

    lax.fori_loop(0, shards, each, 0)
    for a in range(GROUP):
        store(a, turn[a * STRIDE : a * STRIDE + channels, :].T)


def convolve(signal, gate, skip, filt, shards):
    a_loc, inner, channels = signal.shape
    d_loc, n_outer = filt.shape[1:3]
    ch_loc = channels // shards
    half = shards // 2
    d_half = half * d_loc
    f_ch = half * ch_loc
    step = 256
    chunks = n_outer // step
    groups = a_loc // GROUP
    rest = a_loc - GROUP
    d_group = min(GROUP, d_loc)
    inner_scale = 1.0 / math.sqrt(inner)
    outer_scale = 1.0 / math.sqrt(n_outer)
    ahead = min(2, ch_loc)

    def kernel(
        sig_ref, gate_ref, skip_ref, filt_ref, conv_ref, filt_t, part_ref,
        s_buf, f_buf, e_buf, sig_t, outer_t, fwd_t, inv_t, tcb, tbc, r_buf, o_buf,
        l_buf, f_stage, turn, c_buf,
        first_send, first_recv, sig_send, sig_recv, filt_send, filt_recv, ext_send, ext_recv,
        out_send, out_own, out_recv, end_recv, load_sem, stage_sem, tail_sem, part_sem,
    ):
        me = lax.axis_index("seq")
        side = lax.div(me, half)
        mine = lax.rem(me, half)
        barrier = pltpu.get_barrier_semaphore()

        def load_signal(g):
            return pltpu.make_async_copy(
                sig_ref.at[pl.ds(g * GROUP, GROUP)], l_buf.at[g % 2], load_sem.at[g % 2]
            )

        pieces = [
            (p, d, c)
            for p in range(2)
            for d in range(d_loc // d_group)
            for c in range(n_outer // inner)
        ]

        def load_filter(n):
            p, d, c = pieces[n]
            slot = (groups + n) % 2
            return pltpu.make_async_copy(
                filt_ref.at[p, pl.ds(d * d_group, d_group), pl.ds(c * inner, inner)],
                l_buf.at[slot, pl.ds(0, d_group)],
                load_sem.at[slot],
            )

        loads = [(load_signal, g) for g in range(groups)]
        loads += [(load_filter, n) for n in range(len(pieces))]

        def prefetch(n):
            if n < len(loads):
                make, at = loads[n]
                make(at).start()

        prefetch(0)
        prefetch(1)

        def greet(i, carry):
            pl.semaphore_signal(
                barrier, inc=1, device_id={"seq": lax.rem(me + i, shards)}, device_id_type=MESH
            )
            return carry

        lax.fori_loop(1, shards, greet, 0)

        def to_channels(slot, rows, first, count, store, low=0, high=inner // LANES):
            def columns(j, carry):
                lanes = pl.ds(pl.multiple_of(j * LANES, LANES), LANES)
                for r in range(rows):
                    tile = l_buf[slot, r, lanes, :].astype(jnp.float32)
                    turn[pl.ds(r, channels, stride=PITCH), :] = tile.T

                def each(i, carry):
                    for n in range(8):
                        at = pl.multiple_of((first + i * 8 + n) * PITCH, 8)
                        store(i * 8 + n, lanes, turn[pl.ds(at, rows), :].astype(jnp.bfloat16))
                    return carry

                lax.fori_loop(0, count // 8, each, 0)
                return carry

            lax.fori_loop(low, high, columns, 0)

        def turn_signal(g):
            load_signal(g).wait()

            def store(ch, lanes, tile):
                sig_t[ch, g * GROUP : (g + 1) * GROUP, lanes] = tile

            to_channels(g % 2, GROUP, 0, channels, store)
            prefetch(g + 2)

        def rows(s, skip, size):
            return pl.ds(pl.multiple_of(s * a_loc + skip, GROUP), size)

        def group_rows(g):
            return pl.ds(pl.multiple_of(g * GROUP, GROUP), GROUP)

        def own(s):
            return pl.ds(pl.multiple_of(s * ch_loc, ch_loc), ch_loc)

        edge_rows = pl.ds(0, GROUP)
        top = pl.ds(0, GROUP)
        below = pl.ds(GROUP, rest)
        parity = lax.rem(me, 2)
        parts = 2
        width = inner // parts

        def store_first(ch, lanes, tile):
            sig_t[ch, 0:GROUP, lanes] = tile

        load_signal(0).wait()
        for part in range(parts):
            block = pl.ds(part * width, width)

            def send_first(i, carry):
                to = flip(me, (1 - parity) * (shards - i) + parity * i, shards)
                pltpu.make_async_remote_copy(
                    src_ref=sig_t.at[own(to), top, block],
                    dst_ref=s_buf.at[:, rows(me, 0, GROUP), block],
                    send_sem=first_send,
                    recv_sem=first_recv,
                    device_id={"seq": to},
                    device_id_type=MESH,
                ).start()
                return carry

            tiles = width // LANES
            to_channels(0, GROUP, 0, channels, store_first, part * tiles, (part + 1) * tiles)
            if part == 0:
                pl.semaphore_wait(barrier, shards - 1)
            lax.fori_loop(1, shards, send_first, 0)
        prefetch(2)
        pltpu.make_async_copy(
            sig_t.at[own(me), top], s_buf.at[:, rows(me, 0, GROUP)], first_recv
        ).start()

        @pl.when(mine == 0)
        def _():
            def send_ext(i, carry):
                to = (1 - side) * half + i
                pltpu.make_async_remote_copy(
                    src_ref=filt_ref.at[0, 0, edge_rows],
                    dst_ref=e_buf,
                    send_sem=ext_send,
                    recv_sem=ext_recv,
                    device_id={"seq": to},
                    device_id_type=MESH,
                ).start()
                return carry

            lax.fori_loop(0, half, send_ext, 0)

        quarter = half // 2

        def ordered(far, near, middle=None, eager=None):
            def far_loop():
                def one(n, carry):
                    far(half + lax.rem(n, 2) * quarter + lax.div(n, 2))
                    return carry

                lax.fori_loop(0, half, one, 0)

            def near_loop(send, low, high):
                def one(i, carry):
                    send(i)
                    return carry

                lax.fori_loop(low, high, one, 0)

            eager = parity == 0 if eager is None else eager
            pl.when(eager)(far_loop)
            for low, high in ((quarter, half), (1, quarter)):
                if middle is not None:
                    near_loop(middle, low, high)
                near_loop(near, low, high)
            pl.when(jnp.logical_not(eager))(far_loop)

        def send_round(k):
            def send_signal(i):
                to = flip(me, i, shards)
                pltpu.make_async_remote_copy(
                    src_ref=sig_t.at[to * ch_loc + k, below],
                    dst_ref=s_buf.at[k, rows(me, GROUP, rest)],
                    send_sem=sig_send.at[k],
                    recv_sem=sig_recv.at[k],
                    device_id={"seq": to},
                    device_id_type=MESH,
                ).start()

            def send_filter(i):
                to = flip(me, i, shards)
                pltpu.make_async_remote_copy(
                    src_ref=filt_t.at[lax.rem(to, half) * ch_loc + k],
                    dst_ref=f_buf.at[k, :, mine],
                    send_sem=filt_send.at[k],
                    recv_sem=filt_recv.at[k],
                    device_id={"seq": to},
                    device_id_type=MESH,
                ).start()

            def nothing(i):
                return None

            signal_step = send_signal if rest else nothing
            ordered(signal_step, signal_step, send_filter)
            if rest:
                pltpu.make_async_copy(
                    sig_t.at[me * ch_loc + k, below],
                    s_buf.at[k, rows(me, GROUP, rest)],
                    sig_recv.at[k],
                ).start()
            pltpu.make_async_copy(
                filt_t.at[mine * ch_loc + k], f_buf.at[k, :, mine], filt_recv.at[k]
            ).start()

        for g in range(1, groups):
            turn_signal(g)
        def stage(n):
            p, d, c = pieces[n]
            return pltpu.make_async_copy(
                f_stage.at[n % 2],
                filt_t.at[:, p, pl.ds(d * d_group, d_group), pl.ds(c * inner, inner)],
                stage_sem.at[n % 2],
            )

        for n in range(len(pieces)):
            load_filter(n).wait()
            if n >= 2:
                stage(n - 2).wait()

            def store(ch, lanes, tile):
                f_stage[n % 2, ch, :, lanes] = tile

            to_channels((groups + n) % 2, d_group, side * f_ch, f_ch, store)
            prefetch(groups + n + 2)
            stage(n).start()
        for n in range(max(len(pieces) - 2, 0), len(pieces)):
            stage(n).wait()
        for k in range(ahead):
            send_round(k)

        def write_outer(here, i, cos, sin):
            outer_t[here, :] = cos.astype(jnp.bfloat16)
            low = pl.ds(pl.multiple_of(n_outer + i * BASE, BASE), BASE)
            outer_t[low, :] = (-sin).astype(jnp.bfloat16)

        def write_fwd(here, i, cos, sin):
            low = pl.ds(pl.multiple_of(d_half + i * BASE, BASE), BASE)
            fwd_t[here, 0:inner] = cos.astype(jnp.bfloat16)
            fwd_t[here, inner:] = sin.astype(jnp.bfloat16)
            fwd_t[low, 0:inner] = (-sin).astype(jnp.bfloat16)
            fwd_t[low, inner:] = cos.astype(jnp.bfloat16)

        def write_inv(here, i, cos, sin):
            low = pl.ds(pl.multiple_of(inner + i * BASE, BASE), BASE)
            inv_t[here, 0:d_half] = cos.astype(jnp.bfloat16)
            inv_t[here, d_half:] = (-sin).astype(jnp.bfloat16)
            inv_t[low, 0:d_half] = sin.astype(jnp.bfloat16)
            inv_t[low, d_half:] = cos.astype(jnp.bfloat16)

        def write_cb(here, i, cos, sin):
            tcb[0, here, :] = cos * outer_scale
            tcb[1, here, :] = sin * outer_scale

        def write_bc(here, i, cos, sin):
            tbc[0, here, :] = cos * inner_scale
            tbc[1, here, :] = sin * inner_scale

        length = n_outer * inner
        fill(n_outer, n_outer, 0, 0, n_outer, write_outer)
        fill(n_outer, inner, 0, 0, length, write_cb)
        fill(d_half, inner, side * d_half, 0, inner, write_fwd)
        fill(inner, d_half, 0, side * d_half, inner, write_inv)
        fill(inner, n_outer, 0, 0, length, write_bc)

        everything = s_buf.at[:, pl.ds(0, shards * GROUP)]
        pltpu.make_async_copy(everything, everything, first_recv).wait()
        pltpu.make_async_copy(e_buf, e_buf, ext_recv).wait()
        e_row = e_buf[...].astype(jnp.float32)[0:1]

        b_row = lax.broadcasted_iota(jnp.int32, (1, inner), 1)
        b_col = lax.broadcasted_iota(jnp.int32, (inner, 1), 0)
        swing = (1 - side).astype(jnp.float32)
        sign_row = 1.0 - 2.0 * swing * (b_row % 2).astype(jnp.float32)
        sign_col = 1.0 - 2.0 * swing * (b_col % 2).astype(jnp.float32)

        def channel(k, carry):
            slot = lax.rem(k, 2)

            if rest:
                part = s_buf.at[k, pl.ds(0, shards * rest)]
                pltpu.make_async_copy(part, part, sig_recv.at[k]).wait()
            pltpu.make_async_copy(f_buf.at[k], f_buf.at[k], filt_recv.at[k]).wait()
            e_lane = lax.broadcasted_iota(jnp.int32, (1, channels), 1)
            special = jnp.where(e_lane == me * ch_loc + k, e_row, 0.0)
            special = jnp.sum(special, axis=1, keepdims=True)

            @pl.when(k + ahead < ch_loc)
            def _():
                send_round(k + ahead)


            def forward(j, carry):
                at = pl.multiple_of(j * step, step)
                here = pl.ds(at, step)
                x = s_buf[k]
                f_re = matmul(outer_t[here, :], x)
                f_im = matmul(outer_t[pl.ds(pl.multiple_of(n_outer + at, step), step), :], x)
                cos, sin = tcb[0, here, :], tcb[1, here, :]
                q_re = (f_re * cos + f_im * sin).astype(jnp.bfloat16)
                q_im = (f_im * cos - f_re * sin).astype(jnp.bfloat16)
                q = jnp.concatenate([q_re, q_im], axis=1)
                spectrum = matmul_nt(fwd_t[...], q) * inner_scale
                spectrum = spectrum.astype(jnp.bfloat16).astype(jnp.float32)
                s_re, s_im = spectrum[:d_half], spectrum[d_half:]
                h_re = f_buf[k, 0, :, :, here].astype(jnp.float32).reshape(d_half, step)
                h_im = f_buf[k, 1, :, :, here].astype(jnp.float32).reshape(d_half, step)
                d_at = lax.broadcasted_iota(jnp.int32, (d_half, step), 0)
                c_at = lax.broadcasted_iota(jnp.int32, (d_half, step), 1) + at
                share = jnp.where((d_at == 0) & (c_at == 0), 0.5, 1.0)
                product = jnp.concatenate(
                    [(s_re * h_re - s_im * h_im) * share, (s_re * h_im + s_im * h_re) * share],
                    axis=0,
                ).astype(jnp.bfloat16)
                edge = jnp.sum(q_re[0:1].astype(jnp.float32) * sign_row, axis=1, keepdims=True)
                edge = (edge * inner_scale).astype(jnp.bfloat16).astype(jnp.float32)
                edge = (edge * special).astype(jnp.bfloat16).astype(jnp.float32) * 0.5
                c_row = lax.broadcasted_iota(jnp.int32, (1, step), 1) + at
                edge = jnp.where(c_row == 0, edge, 0.0)
                u = matmul(inv_t[...], product)
                u_re, u_im = u[:inner] + sign_col * edge, u[inner:]
                cos, sin = tbc[0, :, here], tbc[1, :, here]
                r_buf[0, :, here] = (u_re * cos - u_im * sin).astype(jnp.bfloat16)
                r_buf[1, :, here] = (u_re * sin + u_im * cos).astype(jnp.bfloat16)
                return carry

            lax.fori_loop(0, chunks, forward, 0)

            @pl.when(k >= 2)
            def _():
                sent = o_buf.at[slot, pl.ds(0, (shards - 1) * a_loc)]
                pltpu.make_async_copy(sent, sent, out_send.at[slot]).wait()
                kept = o_buf.at[slot, pl.ds(0, a_loc)]
                pltpu.make_async_copy(kept, kept, out_own.at[slot]).wait()

            def backward(j, carry):
                at = pl.multiple_of(j * step, step)
                conv = matmul_nt(outer_t[pl.ds(at, step), :], r_buf[0]) + matmul_nt(
                    outer_t[pl.ds(pl.multiple_of(n_outer + at, step), step), :], r_buf[1]
                )
                conv = conv * (2.0 * outer_scale)
                o_buf[slot, pl.ds(at, step), :] = conv.astype(jnp.bfloat16)
                return carry

            lax.fori_loop(0, chunks, backward, 0)
            pltpu.make_async_copy(
                o_buf.at[slot, rows(me, 0, a_loc)], conv_ref.at[me, k], out_own.at[slot]
            ).start()

            def send_out(i):
                to = flip(me, i, shards)
                pltpu.make_async_remote_copy(
                    src_ref=o_buf.at[slot, rows(to, 0, a_loc)],
                    dst_ref=conv_ref.at[me, k],
                    send_sem=out_send.at[slot],
                    recv_sem=out_recv,
                    device_id={"seq": to},
                    device_id_type=MESH,
                ).start()

            def send_end(g, carry):
                def send(i):
                    to = flip(me, i, shards)
                    pltpu.make_async_remote_copy(
                        src_ref=o_buf.at[slot, rows(to, g * GROUP, GROUP)],
                        dst_ref=conv_ref.at[me, k, group_rows(g)],
                        send_sem=out_send.at[slot],
                        recv_sem=end_recv.at[g],
                        device_id={"seq": to},
                        device_id_type=MESH,
                    ).start()

                ordered(send, send, eager=k >= 0)
                return carry

            @pl.when(k < ch_loc - 1)
            def _():
                ordered(send_out, send_out, eager=(parity == 0) | (k >= ch_loc // 2 + 1))

            @pl.when(k == ch_loc - 1)
            def _():
                lax.fori_loop(0, groups, send_end, 0)

            return carry

        def tail_load(g):
            lane = 2 * (g % 2)
            return [
                pltpu.make_async_copy(ref.at[group_rows(g)], l_buf.at[lane + i], tail_sem.at[lane + i])
                for i, ref in enumerate((sig_ref, gate_ref))
            ]

        def tail_store(g):
            return pltpu.make_async_copy(
                l_buf.at[2 * (g % 2) + 1], part_ref.at[group_rows(g)], part_sem.at[g % 2]
            )

        for g in range(min(2, groups - 1)):
            for copy in tail_load(g):
                copy.start()
        lax.fori_loop(0, ch_loc, channel, 0)
        for k in range(max(ch_loc - 2, 0), ch_loc):
            kept = o_buf.at[k % 2, pl.ds(0, a_loc)]
            pltpu.make_async_copy(kept, kept, out_own.at[k % 2]).wait()
        if ch_loc > 1:
            others = conv_ref.at[pl.ds(0, shards - 1), pl.ds(0, ch_loc - 1)]
            pltpu.make_async_copy(others, others, out_recv).wait()

        for g in range(groups):
            landed = conv_ref.at[pl.ds(0, shards - 1), 0, pl.ds(0, GROUP)]
            pltpu.make_async_copy(landed, landed, end_recv.at[g]).wait()
            if g == groups - 1:
                break
            fetch = pltpu.make_async_copy(conv_ref.at[:, :, group_rows(g)], c_buf, tail_sem.at[4])
            fetch.start()
            for copy in tail_load(g):
                copy.wait()
            fetch.wait()
            lane = 2 * (g % 2)

            def columns(j, carry):
                lanes = pl.ds(pl.multiple_of(j * LANES, LANES), LANES)

                def load(t, k):
                    return c_buf[t, k, :, lanes]

                def store(a, conv):
                    full = conv + skip_ref[...] * l_buf[lane, a, lanes, :].astype(jnp.float32)
                    full = l_buf[lane + 1, a, lanes, :].astype(jnp.float32) * full
                    l_buf[lane + 1, a, lanes, :] = full.astype(jnp.bfloat16)

                to_positions(turn, shards, ch_loc, load, store)
                return carry

            lax.fori_loop(0, inner // LANES, columns, 0)
            tail_store(g).start()
            if g + 2 < groups - 1:
                tail_store(g).wait()
                for copy in tail_load(g + 2):
                    copy.start()
        for g in range(max(groups - 3, 0), groups - 1):
            tail_store(g).wait()
        for k in range(max(ch_loc - 2, 0), ch_loc):
            sent = o_buf.at[k % 2, pl.ds(0, (shards - 1) * a_loc)]
            pltpu.make_async_copy(sent, sent, out_send.at[k % 2]).wait()
        sent = sig_t.at[pl.ds(0, (shards - 1) * ch_loc), top]
        pltpu.make_async_copy(sent, sent, first_send).wait()
        for k in range(ch_loc):
            if rest:
                sent = sig_t.at[pl.ds(0, shards - 1), pl.ds(0, rest)]
                pltpu.make_async_copy(sent, sent, sig_send.at[k]).wait()
            sent = filt_t.at[pl.ds(0, half - 1)]
            pltpu.make_async_copy(sent, sent, filt_send.at[k]).wait()

        @pl.when(mine == 0)
        def _():
            sent = filt_ref.at[0, 0, pl.ds(0, half * GROUP)]
            pltpu.make_async_copy(sent, sent, ext_send).wait()

    anywhere = pl.BlockSpec(memory_space=pl.ANY)
    bf16, f32 = jnp.bfloat16, jnp.float32
    per_channel = pltpu.SemaphoreType.DMA((ch_loc,))
    single = pltpu.SemaphoreType.DMA
    pair = pltpu.SemaphoreType.DMA((2,))
    return pl.pallas_call(
        kernel,
        out_shape=(
            jax.ShapeDtypeStruct((shards, ch_loc, a_loc, inner), bf16),
            jax.ShapeDtypeStruct((f_ch, 2, d_loc, n_outer), bf16),
            jax.ShapeDtypeStruct((max(rest, GROUP), inner, channels), bf16),
        ),
        in_specs=[anywhere, anywhere, pl.BlockSpec(memory_space=pltpu.VMEM), anywhere],
        out_specs=(anywhere, anywhere, anywhere),
        scratch_shapes=[
            pltpu.VMEM((ch_loc, n_outer, inner), bf16),
            pltpu.VMEM((ch_loc, 2, half, d_loc, n_outer), bf16),
            pltpu.VMEM((GROUP, channels), bf16),
            pltpu.VMEM((channels, a_loc, inner), bf16),
            pltpu.VMEM((2 * n_outer, n_outer), bf16),
            pltpu.VMEM((2 * d_half, 2 * inner), bf16),
            pltpu.VMEM((2 * inner, 2 * d_half), bf16),
            pltpu.VMEM((2, n_outer, inner), f32),
            pltpu.VMEM((2, inner, n_outer), f32),
            pltpu.VMEM((2, inner, n_outer), bf16),
            pltpu.VMEM((2, n_outer, inner), bf16),
            pltpu.VMEM((4, GROUP, inner, channels), bf16),
            pltpu.VMEM((2, f_ch, d_group, inner), bf16),
            pltpu.VMEM((channels * PITCH, LANES), f32),
            pltpu.VMEM((shards, ch_loc, GROUP, inner), bf16),
            single,
            single,
            per_channel,
            per_channel,
            per_channel,
            per_channel,
            single,
            single,
            pair,
            pair,
            single,
            pltpu.SemaphoreType.DMA((groups,)),
            pair,
            pair,
            pltpu.SemaphoreType.DMA((5,)),
            pair,
        ],
        compiler_params=pltpu.CompilerParams(
            collective_id=0, has_side_effects=True, vmem_limit_bytes=67043328
        ),
        name="convolve",
    )(signal, gate, skip, filt)


def finish(convolved, part, signal, gate, skip):
    a_loc, inner, channels = signal.shape
    shards, ch_loc = convolved.shape[:2]
    done = a_loc - GROUP
    copies = done // GROUP
    chunks = inner // LANES

    def kernel(
        conv_ref, part_ref, sig_ref, gate_ref, skip_ref, out_ref,
        c_buf, s_buf, g_buf, p_buf, turn, in_sem, part_in, part_out, out_sem,
    ):
        last = pl.ds(done, GROUP)
        loads = []
        for j in range(chunks):
            lanes = pl.ds(j * LANES, LANES)
            loads.append(
                [
                    pltpu.make_async_copy(
                        conv_ref.at[:, :, last, lanes], c_buf.at[:, :, :, lanes], in_sem.at[0, j]
                    ),
                    pltpu.make_async_copy(
                        sig_ref.at[last, lanes], s_buf.at[:, lanes], in_sem.at[1, j]
                    ),
                    pltpu.make_async_copy(
                        gate_ref.at[last, lanes], g_buf.at[:, lanes], in_sem.at[2, j]
                    ),
                ]
            )
            for copy in loads[-1]:
                copy.start()
        moves = []
        for n in range(copies):
            rows = pl.ds(n * GROUP, GROUP)
            moves.append(
                (
                    pltpu.make_async_copy(part_ref.at[rows], p_buf.at[n], part_in.at[n]),
                    pltpu.make_async_copy(p_buf.at[n], out_ref.at[rows], part_out.at[n]),
                )
            )
        stores = []
        for j in range(chunks):
            lanes = pl.ds(j * LANES, LANES)

            def load(t, k):
                return c_buf[t, k, :, lanes]

            def store(a, conv):
                full = conv + skip_ref[...] * s_buf[a, lanes, :].astype(jnp.float32)
                full = g_buf[a, lanes, :].astype(jnp.float32) * full
                g_buf[a, lanes, :] = full.astype(jnp.bfloat16)

            for copy in loads[j]:
                copy.wait()
            if j == 0:
                for move in moves:
                    move[0].start()
            to_positions(turn, shards, ch_loc, load, store)
            stores.append(
                pltpu.make_async_copy(
                    g_buf.at[:, lanes], out_ref.at[last, lanes], out_sem.at[j]
                )
            )
            stores[-1].start()
            if j < copies:
                moves[j][0].wait()
                moves[j][1].start()
        for n in range(chunks, copies):
            moves[n][0].wait()
            moves[n][1].start()
        for copy in stores + [move[1] for move in moves]:
            copy.wait()

    anywhere = pl.BlockSpec(memory_space=pl.ANY)
    rows_shape = (GROUP, inner, channels)
    return pl.pallas_call(
        kernel,
        out_shape=jax.ShapeDtypeStruct(signal.shape, jnp.bfloat16),
        in_specs=[anywhere] * 4 + [pl.BlockSpec(memory_space=pltpu.VMEM)],
        out_specs=anywhere,
        scratch_shapes=[
            pltpu.VMEM((shards, ch_loc, GROUP, inner), jnp.bfloat16),
            pltpu.VMEM(rows_shape, jnp.bfloat16),
            pltpu.VMEM(rows_shape, jnp.bfloat16),
            pltpu.VMEM((max(copies, 1), *rows_shape), jnp.bfloat16),
            pltpu.VMEM((GROUP * STRIDE, LANES), jnp.float32),
            pltpu.SemaphoreType.DMA((3, chunks)),
            pltpu.SemaphoreType.DMA((max(copies, 1),)),
            pltpu.SemaphoreType.DMA((max(copies, 1),)),
            pltpu.SemaphoreType.DMA((chunks,)),
        ],
        compiler_params=pltpu.CompilerParams(vmem_limit_bytes=67043328),
        name="finish",
    )(convolved, part, signal, gate, skip)


def local(signal, gate_values, skip_gain, filter_spectrum):
    shards = lax.axis_size("seq")
    positions, channels = signal.shape
    d_loc, n_outer = filter_spectrum.shape[1:3]
    grid = (n_outer // shards, d_loc * shards, channels)
    signal, gate = signal.reshape(grid), gate_values.reshape(grid)
    skip = skip_gain.reshape(1, channels)
    convolved, _, part = convolve(signal, gate, skip, filter_spectrum, shards)
    result = finish(convolved, part, signal, gate, skip)
    return result.reshape(positions, channels)


def solution(mesh):
    return jax.shard_map(
        local,
        mesh=mesh,
        in_specs=(P("seq", "chan"), P("seq", "chan"), P("chan"), P(None, "seq", None, "chan")),
        out_specs=P("seq", "chan"),
        check_vma=False,
    )
```
